32 devices in a mesh: dp: 8 (over z, core), tensor: 4 (over y, x).
Axes of the slice: x: 2, y: 2, z: 4, core: 2. Of those that a mesh axis runs over, the one named last changes fastest.
Arguments:
- token_ids: int32 [8, 1024], P('dp', 'tensor'), may hold values from 0 to 30527
- lengths: int32 [8], P('dp'), may hold values from 256 to 1024, as said below
- teacher_bins: int32 [8], P('dp'), may hold values from 0 to 127
- embed_table: bfloat16 [30528, 1024], P('tensor'), may hold values from -6 to 6
- query_key_value_matrix: bfloat16 [1024, 3, 1024], P('dp', None, 'tensor'), may hold values from -2 to 2
- output_matrix: bfloat16 [1024, 1024], P('tensor', 'dp'), may hold values from -0.1875 to 0.1875
- up_matrix: bfloat16 [1024, 4096], P('dp', 'tensor'), may hold values from -0.1875 to 0.1875
- down_matrix: bfloat16 [4096, 1024], P('tensor', 'dp'), may hold values from -0.09375 to 0.09375
- w_head: bfloat16 [1024, 128], P('dp'), may hold values from -64 to 64
Outputs:
- loss: float32 [], replicated
- query_key_value_gradient: float32 [1024, 3, 1024], P('dp', None, 'tensor')
- output_weight_gradient: float32 [1024, 1024], P('tensor', 'dp')
- up_weight_gradient: float32 [1024, 4096], P('dp', 'tensor')
- down_weight_gradient: float32 [4096, 1024], P('tensor', 'dp')
- grad_head: float32 [1024, 128], P('dp')
The draws below stay inside these ranges and needn't reach their ends.
Inputs may be any that keep to these rules, and one draw needn't show every extreme that they name: lengths[0] is 1024.
All inputs are finite; a program needn't handle non-finite values.
Results may differ from the reference program's by a relative error of at most 0.02.
Values may be sent and summed in bfloat16 or wider, within the bound.
A program may use at most 128 MiB of HBM per device.

```python
import math
import jax
import jax.numpy as jnp
import numpy as np
from jax import lax

D = 1024
HEAD_COUNT = 16
HEAD_WIDTH = 64
FF = 4096
VOCAB = 30528
NBINS = 128
LEN = 1024
SEQS = 8
N_TENSOR = 4


def draw_lengths(key, part):
    values = jax.random.randint(jax.random.fold_in(key, 11), (SEQS,), LEN // 4, LEN + 1, dtype=jnp.int32)
    return values.at[0].set(LEN)


def draw_embed_table(key, part):
    normal_rows = jax.random.normal(jax.random.fold_in(key, 21), (VOCAB, D), jnp.float32)
    values = normal_rows
    return jnp.clip(values, -6.0, 6.0).astype(jnp.bfloat16)


def draw_query_key_value_matrix(key, part):
    scaled = jnp.clip(jax.random.normal(jax.random.fold_in(key, 31), (D, 3, D), jnp.float32), -6.0, 6.0) * (1.0 / math.sqrt(D))
    return jnp.clip(scaled, -2.0, 2.0).astype(jnp.bfloat16)


def draw_w_head(key, part):
    drawn_cols = jnp.clip(jax.random.normal(jax.random.fold_in(key, 41), (D, NBINS), jnp.float32), -6.0, 6.0) * 0.1
    return jnp.clip(drawn_cols, -64.0, 64.0).astype(jnp.bfloat16)


def plant(entries, rng, least, top_value):
    longest = entries.shape.index(max(entries.shape))
    spots = []
    for shift in (0, 1):
        where = [jax.random.randint(jax.random.fold_in(rng, axis), (), 0, length) for axis, length in enumerate(entries.shape)]
        where[longest] = (where[longest] + shift) % entries.shape[longest]
        spots.append(tuple(where))
    return entries.at[spots[0]].set(least).at[spots[1]].set(top_value)


def shard_levels(own_key, extent, cuts, smallest, high):
    def one(axis_at, parts):
        heights = jax.random.uniform(jax.random.fold_in(jax.random.fold_in(own_key, 6), axis_at), (parts,), jnp.float32, smallest / len(cuts), high / len(cuts))
        return jnp.repeat(jnp.exp(heights), extent[axis_at] // parts).reshape((-1,) + (1,) * (len(extent) - axis_at - 1))

    loudness = one(*cuts[0])
    for cut in cuts[1:]:
        loudness = loudness * one(*cut)
    return loudness


def rank_table(amount, slope):
    portions = [(1 << 20) // math.isqrt(standing ** slope) + 1 for standing in range(1, amount + 1)]
    scale = 1 + sum(portions) // (1 << 30)
    return np.cumsum(np.array([max(1, weight // scale) for weight in portions]))


def skewed_ids(stream_key, extent, amount, lean):
    listing = rank_table(amount, lean)
    ticket = jax.random.randint(jax.random.fold_in(stream_key, 1), extent, 0, int(listing[amount - 1]))
    rank = jnp.searchsorted(jnp.asarray(listing, jnp.int32), ticket, side="right")
    return jax.random.permutation(jax.random.fold_in(stream_key, 2), amount)[rank].astype(jnp.int32)


def normal_values(key, shape, scale, reach, shards=(), held_as=jnp.bfloat16):
    values = jax.random.normal(key, shape, jnp.float32) * scale
    if len(shards) > 0:
        values = shard_levels(key, shape, shards, -0.22, 0.18) * values
    return jnp.clip(values, min=-reach, max=reach).astype(held_as)


def setup_inputs(seed: int = 0) -> dict:
    streams_of = jax.random.split(jax.random.key(seed), 10)
    token_ids = plant(skewed_ids(streams_of[0], (SEQS, LEN), VOCAB, 2), jax.random.fold_in(streams_of[0], 3), 0, VOCAB - 1).astype(jnp.int32)
    lengths = draw_lengths(jax.random.fold_in(streams_of[9], 71), 0)
    teacher_bins = plant(jax.random.randint(streams_of[2], (SEQS,), 0, NBINS), jax.random.fold_in(streams_of[2], 1), 0, NBINS - 1).astype(jnp.int32)
    embed_table = draw_embed_table(jax.random.fold_in(streams_of[9], 71), 0)
    query_key_value_matrix = draw_query_key_value_matrix(jax.random.fold_in(streams_of[9], 71), 0)
    output_matrix = normal_values(streams_of[5], (D, D), D ** -0.5, 0.1875, ((0, 4), (1, 8)))
    up_matrix = normal_values(streams_of[6], (D, FF), D ** -0.5, 0.1875, ((0, 8), (1, 4)))
    down_matrix = normal_values(streams_of[7], (FF, D), FF ** -0.5, 0.09375, ((0, 4), (1, 8)))
    w_head = draw_w_head(jax.random.fold_in(streams_of[9], 71), 0)
    return dict(token_ids=token_ids, lengths=lengths, teacher_bins=teacher_bins, embed_table=embed_table, query_key_value_matrix=query_key_value_matrix, output_matrix=output_matrix, up_matrix=up_matrix, down_matrix=down_matrix, w_head=w_head)


EPS = 1e-05

def normalize(values):
    mean = lax.optimization_barrier(jnp.mean(values, axis=-1, keepdims=True))
    centered = values - mean
    return centered * lax.rsqrt(lax.optimization_barrier(jnp.mean(centered * centered, axis=-1, keepdims=True)) + EPS)

def gelu_tanh(values):
    return 0.5 * values * (1.0 + jnp.tanh(0.7978845608028654 * (values + 0.044715 * values * values * values)))

def attend(query, keys, values_in, lengths):
    scale = query.shape[-1] ** (-0.5)
    scores = jnp.einsum('sqhe,skhe->shqk', query, keys) * scale
    visible = jnp.arange(keys.shape[1], dtype=jnp.int32)[None, :] < lengths[:, None]
    scores = jnp.where(visible[:, None, None, :], scores, -1e+30)
    top = lax.optimization_barrier(jnp.max(scores, axis=-1, keepdims=True))
    expo = jnp.exp(scores - top)
    probs = expo / lax.optimization_barrier(jnp.sum(expo, axis=-1, keepdims=True))
    rounded = lax.optimization_barrier(probs.astype(jnp.bfloat16)).astype(jnp.float32)
    return jnp.einsum('shqk,skhe->sqhe', rounded, values_in)

def rounded_sum(left_operand, right_operand, blocks, inner_value):
    total = None
    for layer_block in range(blocks):
        slice_portion = jnp.einsum('wou,ue->woe', left_operand[:, :, layer_block * inner_value:(layer_block + 1) * inner_value].astype(jnp.float32), right_operand[layer_block * inner_value:(layer_block + 1) * inner_value].astype(jnp.float32))
        slice_portion = lax.optimization_barrier(slice_portion.astype(jnp.bfloat16)).astype(jnp.float32)
        total = slice_portion if total is None else total + slice_portion
    return total

def reference(token_ids, lengths, teacher_bins, embed_table, query_key_value_matrix, output_matrix, up_matrix, down_matrix, w_head):
    sequence_batch, sequence_length = token_ids.shape
    width = embed_table.shape[1]
    first = jnp.take(embed_table, token_ids, axis=0)
    first_normed_rows = normalize(first.astype(jnp.float32)).astype(jnp.bfloat16)
    mixed_output = jnp.einsum('fxw,wvr->fxvr', first_normed_rows.astype(jnp.float32), query_key_value_matrix.astype(jnp.float32)).astype(jnp.bfloat16)
    split = mixed_output.astype(jnp.float32).reshape(sequence_batch, sequence_length, 3, HEAD_COUNT, HEAD_WIDTH)

    def forward_one(item):
        query, keys, vals, count = item
        return attend(query[None], keys[None], vals[None], count[None])[0]
    attended_rows = lax.map(forward_one, (split[:, :, 0], split[:, :, 1], split[:, :, 2], lengths))
    attended_rows = attended_rows.astype(jnp.bfloat16).reshape(sequence_batch, sequence_length, width)
    attn = rounded_sum(attended_rows, output_matrix, N_TENSOR, width // N_TENSOR)
    second = (first.astype(jnp.float32) + attn).astype(jnp.bfloat16)
    second_normed_rows = normalize(second.astype(jnp.float32)).astype(jnp.bfloat16)
    hidden_preactivation = jnp.einsum('ntp,pk->ntk', second_normed_rows.astype(jnp.float32), up_matrix.astype(jnp.float32))
    hidden_activated = gelu_tanh(hidden_preactivation).astype(jnp.bfloat16)
    ffn = rounded_sum(hidden_activated, down_matrix, N_TENSOR, FF // N_TENSOR)
    third = second.astype(jnp.float32) + ffn
    live = (jnp.arange(sequence_length, dtype=jnp.int32)[None, :] < lengths[:, None]).astype(jnp.float32)
    counts = lengths.astype(jnp.float32)[:, None]
    pooled = lax.optimization_barrier(jnp.sum(third * live[:, :, None], axis=1)) / counts
    final, final_back = jax.vjp(normalize, pooled)
    head = w_head.astype(jnp.float32)
    logits = jnp.dot(final, head, precision=lax.Precision.HIGHEST)
    top = lax.optimization_barrier(jnp.max(logits, axis=-1, keepdims=True))
    total_exp = jnp.log(lax.optimization_barrier(jnp.sum(jnp.exp(logits - top), axis=-1, keepdims=True))) + top
    labels = (teacher_bins[:, None] == jnp.arange(logits.shape[1], dtype=jnp.int32)[None, :]).astype(jnp.float32)
    losses = total_exp[:, 0] - lax.optimization_barrier(jnp.sum(logits * labels, axis=-1))
    loss = jnp.sum(losses) / sequence_batch
    g_logits = (jnp.exp(logits - total_exp) - labels) / sequence_batch
    grad_head = jnp.dot(final.T, g_logits, precision=lax.Precision.HIGHEST)
    g_final = jnp.dot(g_logits, head.T, precision=lax.Precision.HIGHEST)
    g_pooled = final_back(g_final)[0]
    per_token = g_pooled / counts
    g_third = per_token[:, None, :] * live[:, :, None]
    third_gradient_batch = g_third.astype(jnp.bfloat16)
    down_weight_gradient = jnp.einsum('omi,omy->iy', hidden_activated.astype(jnp.float32), third_gradient_batch.astype(jnp.float32))
    hidden_gradient = jnp.einsum('tpu,bu->tpb', third_gradient_batch.astype(jnp.float32), down_matrix.astype(jnp.float32))
    gelu_back = jax.vjp(gelu_tanh, hidden_preactivation)[1]
    preact_gradient = gelu_back(hidden_gradient)[0].astype(jnp.bfloat16)
    up_weight_gradient = jnp.einsum('qon,qom->nm', second_normed_rows.astype(jnp.float32), preact_gradient.astype(jnp.float32))
    g_normed_two = rounded_sum(preact_gradient, up_matrix.T, N_TENSOR, FF // N_TENSOR)
    norm_back = jax.vjp(normalize, second.astype(jnp.float32))[1]
    second_gradient = (g_third + norm_back(g_normed_two)[0]).astype(jnp.bfloat16)
    output_weight_gradient = jnp.einsum('jxm,jxn->mn', attended_rows.astype(jnp.float32), second_gradient.astype(jnp.float32))
    attended_gradient = jnp.einsum('kmi,qi->kmq', second_gradient.astype(jnp.float32), output_matrix.astype(jnp.float32)).reshape(sequence_batch, sequence_length, HEAD_COUNT, HEAD_WIDTH)

    def backward_one(item):
        query, keys, vals, count, grad = item
        back = jax.vjp(lambda a, b, c: attend(a[None], b[None], c[None], count[None])[0], query, keys, vals)[1]
        return back(grad)
    g_query, g_keys, g_vals = lax.map(backward_one, (split[:, :, 0], split[:, :, 1], split[:, :, 2], lengths, attended_gradient))
    mixed_gradient = jnp.stack([g_query, g_keys, g_vals], axis=2).reshape(sequence_batch, sequence_length, 3, width).astype(jnp.bfloat16)
    query_key_value_gradient = jnp.einsum('rvt,rvzx->tzx', first_normed_rows.astype(jnp.float32), mixed_gradient.astype(jnp.float32))
    return (loss, query_key_value_gradient, output_weight_gradient, up_weight_gradient, down_weight_gradient, grad_head)
```

```python
import functools

import jax
import jax.numpy as jnp
from jax import lax
from jax.experimental import pallas as pl
from jax.experimental.pallas import tpu as pltpu
from jax.sharding import PartitionSpec as P

HEAD_WIDTH = 64
EPS = 1e-05
BF = jnp.bfloat16
F32 = jnp.float32
MESH = pl.DeviceIdType.MESH
VMEM = pltpu.VMEM
BIG = 60 * 1024 * 1024


def normalize(values):
    mean = jnp.mean(values, axis=-1, keepdims=True)
    centered = values - mean
    return centered * lax.rsqrt(jnp.mean(centered * centered, axis=-1, keepdims=True) + EPS)


def vmem_spec():
    return pl.BlockSpec(memory_space=pltpu.VMEM)


def greet(axis, count):
    me = lax.axis_index(axis)
    barrier = pltpu.get_barrier_semaphore()
    for step in range(1, count):
        pl.semaphore_signal(
            barrier, inc=1, device_id={axis: lax.rem(me + step, count)}, device_id_type=MESH
        )
    pl.semaphore_wait(barrier, count - 1)
    return me


def gather_body(axis, count, x_ref, out_ref, send_sem, recv_sem):
    me = greet(axis, count)
    copies = []
    for step in range(1, count):
        copy = pltpu.make_async_remote_copy(
            src_ref=x_ref,
            dst_ref=out_ref.at[me],
            send_sem=send_sem.at[step - 1],
            recv_sem=recv_sem.at[step - 1],
            device_id={axis: lax.rem(me + step, count)},
            device_id_type=MESH,
        )
        copy.start()
        copies.append(copy)
    out_ref[me] = x_ref[...]
    for copy in copies:
        copy.wait()


def gather_all(x, axis, count, ident):
    return pl.pallas_call(
        functools.partial(gather_body, axis, count),
        out_shape=jax.ShapeDtypeStruct((count,) + x.shape, x.dtype),
        in_specs=[vmem_spec()],
        out_specs=vmem_spec(),
        scratch_shapes=[
            pltpu.SemaphoreType.DMA((count - 1,)),
            pltpu.SemaphoreType.DMA((count - 1,)),
        ],
        compiler_params=pltpu.CompilerParams(collective_id=ident, has_side_effects=True),
        name="gather_all",
    )(x)


def scatter_phase(axis, count, me, x_ref, held, send_sem, recv_sem, put):
    copies = []
    for step in range(1, count):
        peer = lax.rem(me + step, count)
        copy = pltpu.make_async_remote_copy(
            src_ref=x_ref.at[peer],
            dst_ref=held.at[step - 1],
            send_sem=send_sem.at[step - 1],
            recv_sem=recv_sem.at[step - 1],
            device_id={axis: peer},
            device_id_type=MESH,
        )
        copy.start()
        copies.append(copy)
    for copy in copies:
        copy.wait()
    rows = x_ref.shape[1]
    tile = 32

    def add(index, carry):
        at = pl.ds(pl.multiple_of(index * tile, tile), tile)
        total = x_ref[me, at].astype(F32)
        for step in range(1, count):
            total = total + held[step - 1, at].astype(F32)
        put(at, total)
        return carry

    lax.fori_loop(0, rows // tile, add, 0)


def reduce_body(axis, count, x_ref, out_ref, held, send_sem, recv_sem):
    me = greet(axis, count)

    def put(at, total):
        out_ref[at] = total.astype(out_ref.dtype)

    scatter_phase(axis, count, me, x_ref, held, send_sem, recv_sem, put)


def reduce_scatter(x, axis, count, ident):
    return pl.pallas_call(
        functools.partial(reduce_body, axis, count),
        out_shape=jax.ShapeDtypeStruct(x.shape[1:], x.dtype),
        in_specs=[vmem_spec()],
        out_specs=vmem_spec(),
        scratch_shapes=[
            VMEM((count - 1,) + x.shape[1:], x.dtype),
            pltpu.SemaphoreType.DMA((count - 1,)),
            pltpu.SemaphoreType.DMA((count - 1,)),
        ],
        compiler_params=pltpu.CompilerParams(collective_id=ident, has_side_effects=True),
        name="reduce_scatter",
    )(x)


def sum_all_body(axis, count, x_ref, out_ref, held, send_sem, recv_sem, send_two, recv_two):
    me = greet(axis, count)

    def put(at, total):
        out_ref[me, at] = total.astype(out_ref.dtype)

    scatter_phase(axis, count, me, x_ref, held, send_sem, recv_sem, put)
    copies = []
    for step in range(1, count):
        copy = pltpu.make_async_remote_copy(
            src_ref=out_ref.at[me],
            dst_ref=out_ref.at[me],
            send_sem=send_two.at[step - 1],
            recv_sem=recv_two.at[step - 1],
            device_id={axis: lax.rem(me + step, count)},
            device_id_type=MESH,
        )
        copy.start()
        copies.append(copy)
    for copy in copies:
        copy.wait()


def sum_all(x, axis, count, ident):
    return pl.pallas_call(
        functools.partial(sum_all_body, axis, count),
        out_shape=jax.ShapeDtypeStruct(x.shape, x.dtype),
        in_specs=[vmem_spec()],
        out_specs=vmem_spec(),
        scratch_shapes=[VMEM((count - 1,) + x.shape[1:], x.dtype)]
        + [pltpu.SemaphoreType.DMA((count - 1,))] * 4,
        compiler_params=pltpu.CompilerParams(collective_id=ident, has_side_effects=True),
        name="sum_all",
    )(x)


def contract(left, right, dims):
    return lax.dot_general(left, right, ((dims[:1], dims[1:]), ((), ())), preferred_element_type=F32)


def masked_scores(keys, query, length):
    scores = contract(keys, query, (0, 0))
    position = lax.broadcasted_iota(jnp.int32, scores.shape, 0)
    return jnp.where(position < length, scores, -1e30)


def attend_body(chunk, length_ref, qkv_ref, out_ref, lse_ref):
    length = length_ref[0]
    keys, vals = qkv_ref[1], qkv_ref[2]
    scale = HEAD_WIDTH ** (-0.5)
    for at in range(0, qkv_ref.shape[2], chunk):
        query = (qkv_ref[0, :, at : at + chunk].astype(F32) * scale).astype(BF)
        scores = masked_scores(keys, query, length)
        top = jnp.max(scores, axis=0, keepdims=True)
        expo = jnp.exp(scores - top)
        total = jnp.sum(expo, axis=0, keepdims=True)
        mixed = contract(vals, expo.astype(BF), (1, 0))
        out_ref[:, at : at + chunk] = (mixed * (1.0 / total)).astype(BF)
        lse_ref[0, :, at : at + chunk] = top + jnp.log(total)


def attend(qkv, lengths, chunk):
    _, width, length = qkv.shape
    heads = width // HEAD_WIDTH
    return pl.pallas_call(
        functools.partial(attend_body, chunk),
        grid=(heads,),
        out_shape=(
            jax.ShapeDtypeStruct((width, length), BF),
            jax.ShapeDtypeStruct((heads, 1, length), F32),
        ),
        in_specs=[
            pl.BlockSpec(memory_space=pltpu.SMEM),
            pl.BlockSpec((3, HEAD_WIDTH, length), lambda h: (0, h, 0)),
        ],
        out_specs=(
            pl.BlockSpec((HEAD_WIDTH, length), lambda h: (h, 0)),
            pl.BlockSpec((1, 1, length), lambda h: (h, 0, 0)),
        ),
        cost_estimate=pl.CostEstimate(
            flops=4 * width * length * length,
            bytes_accessed=8 * width * length,
            transcendentals=heads * length * length,
        ),
        compiler_params=pltpu.CompilerParams(vmem_limit_bytes=BIG),
        name="attend",
    )(lengths, qkv)


def attend_back_body(chunk, length_ref, qkv_ref, lse_ref, grad_ref, out_ref):
    length = length_ref[0]
    keys, vals = qkv_ref[1], qkv_ref[2]
    scale = HEAD_WIDTH ** (-0.5)
    span = qkv_ref.shape[2]
    g_keys = jnp.zeros((HEAD_WIDTH, span), F32)
    g_vals = jnp.zeros((HEAD_WIDTH, span), F32)
    for at in range(0, span, chunk):
        here = slice(at, at + chunk)
        query = (qkv_ref[0, :, here].astype(F32) * scale).astype(BF)
        grad = grad_ref[:, here]
        probs = jnp.exp(masked_scores(keys, query, length) - lse_ref[0, :, here])
        g_probs = contract(vals, grad, (0, 0))
        weighted = probs * g_probs
        inner = jnp.sum(weighted, axis=0, keepdims=True)
        g_scores = (weighted - probs * inner).astype(BF)
        out_ref[0, :, here] = (contract(keys, g_scores, (1, 0)) * scale).astype(BF)
        g_keys += contract(query, g_scores, (1, 1))
        g_vals += contract(grad, probs.astype(BF), (1, 1))
    out_ref[1] = g_keys.astype(BF)
    out_ref[2] = g_vals.astype(BF)


def attend_back(qkv, lengths, lse, grad, chunk):
    _, width, length = qkv.shape
    heads = width // HEAD_WIDTH
    return pl.pallas_call(
        functools.partial(attend_back_body, chunk),
        grid=(heads,),
        out_shape=jax.ShapeDtypeStruct(qkv.shape, BF),
        in_specs=[
            pl.BlockSpec(memory_space=pltpu.SMEM),
            pl.BlockSpec((3, HEAD_WIDTH, length), lambda h: (0, h, 0)),
            pl.BlockSpec((1, 1, length), lambda h: (h, 0, 0)),
            pl.BlockSpec((HEAD_WIDTH, length), lambda h: (h, 0)),
        ],
        out_specs=pl.BlockSpec((3, HEAD_WIDTH, length), lambda h: (0, h, 0)),
        cost_estimate=pl.CostEstimate(
            flops=10 * width * length * length,
            bytes_accessed=14 * width * length,
            transcendentals=heads * length * length,
        ),
        compiler_params=pltpu.CompilerParams(vmem_limit_bytes=BIG),
        name="attend_back",
    )(lengths, qkv, lse, grad)


def hidden_body(length_ref, normed_ref, up_ref, slope_ref, sum_ref):
    pre = jnp.dot(normed_ref[...], up_ref[...], preferred_element_type=F32)
    live = lax.broadcasted_iota(jnp.int32, pre.shape, 0) < length_ref[0]
    square = pre * pre
    bend = jnp.tanh(0.7978845608028654 * (pre * (1.0 + 0.044715 * square)))
    half = 0.5 * (1.0 + bend)
    act = (pre * half).astype(BF).astype(F32)
    sum_ref[...] = jnp.sum(jnp.where(live, act, 0.0), axis=0, keepdims=True)
    inner = 0.7978845608028654 * (1.0 + 3 * 0.044715 * square)
    slope = half + 0.5 * pre * (1.0 - bend * bend) * inner
    slope_ref[...] = jnp.where(live, slope, 0.0).astype(BF)


def hidden(normed, up, lengths, chunk):
    length, width = normed.shape
    units = up.shape[1]
    return pl.pallas_call(
        hidden_body,
        grid=(units // chunk,),
        out_shape=(
            jax.ShapeDtypeStruct((length, units), BF),
            jax.ShapeDtypeStruct((1, units), F32),
        ),
        in_specs=[
            pl.BlockSpec(memory_space=pltpu.SMEM),
            pl.BlockSpec((length, width), lambda f: (0, 0)),
            pl.BlockSpec((width, chunk), lambda f: (0, f)),
        ],
        out_specs=(
            pl.BlockSpec((length, chunk), lambda f: (0, f)),
            pl.BlockSpec((1, chunk), lambda f: (0, f)),
        ),
        cost_estimate=pl.CostEstimate(
            flops=2 * length * width * units,
            bytes_accessed=6 * length * units,
            transcendentals=length * units,
        ),
        compiler_params=pltpu.CompilerParams(vmem_limit_bytes=BIG),
        name="hidden",
    )(lengths, normed, up)


def per_device(
    token_ids,
    lengths,
    teacher_bins,
    embed_table,
    query_key_value_matrix,
    output_matrix,
    up_matrix,
    down_matrix,
    w_head,
):
    ranks = lax.axis_size("tensor")
    groups = lax.axis_size("dp")
    rank = lax.axis_index("tensor")
    group = lax.axis_index("dp")
    assert token_ids.shape[0] == 1
    local_len = token_ids.shape[1]
    span = local_len * ranks
    vocab_local, width = embed_table.shape
    d_local, _, e_local = query_key_value_matrix.shape
    f_local = up_matrix.shape[1]
    bins = w_head.shape[1]
    exact = lax.Precision.HIGHEST

    qkv_full = lax.all_gather(
        query_key_value_matrix.reshape(d_local, 3 * e_local), "dp", axis=0, tiled=True
    )
    out_parts = lax.all_gather(output_matrix, ("tensor", "dp"), axis=0, tiled=False)
    out_full = (
        out_parts.reshape(ranks, groups, e_local, d_local)
        .transpose(0, 2, 1, 3)
        .reshape(ranks * e_local, width)
    )
    up_full = lax.all_gather(up_matrix, "dp", axis=0, tiled=True)
    low = lax.all_gather(
        jnp.concatenate([down_matrix, w_head.reshape(bins, d_local)], axis=0), "dp", axis=0, tiled=False
    )
    down_full = low[:, :f_local]
    head_wide = low[:, f_local:].reshape(width, bins).astype(F32)

    all_ids = gather_all(token_ids, "tensor", ranks, 1).reshape(ranks, local_len)
    shifted = all_ids - rank * vocab_local
    inside = (shifted >= 0) & (shifted < vocab_local)
    rows = jnp.take(embed_table, jnp.clip(shifted, 0, vocab_local - 1), axis=0)
    first = sum_all(
        jnp.where(inside[..., None], rows, jnp.zeros((), BF)), "tensor", ranks, 2
    ).reshape(span, width)
    normed_one = normalize(first.astype(F32)).astype(BF)
    qkv = (
        lax.dot_general(qkv_full, normed_one, (((0,), (1,)), ((), ())), preferred_element_type=F32)
        .astype(BF)
        .reshape(3, e_local, span)
    )
    chunk = min(256, span)
    context, lse = attend(qkv, lengths, chunk)
    context_all = gather_all(context, "tensor", ranks, 3).reshape(ranks * e_local, span)
    attn = lax.dot_general(
        context_all, out_full, (((0,), (0,)), ((), ())), preferred_element_type=F32
    )
    second = (first.astype(F32) + attn).astype(BF)
    normed_f, norm_back = jax.vjp(normalize, second.astype(F32))
    normed_two = normed_f.astype(BF)
    slope, hidden_sum = hidden(normed_two, up_full, lengths, min(256, f_local))

    live = (jnp.arange(span, dtype=jnp.int32) < lengths[0]).astype(F32)
    count = lengths.astype(F32)[:, None]
    ffn_part = jnp.einsum(
        "of,jfd->ojd", hidden_sum, down_full.astype(F32), precision=exact
    ).reshape(1, width)
    ffn_all = gather_all(ffn_part, "tensor", ranks, 4)
    second_sum = jnp.sum(second.astype(F32) * live[:, None], axis=0, keepdims=True)
    pooled = (second_sum + jnp.sum(ffn_all, axis=0)) / count
    final, final_back = jax.vjp(normalize, pooled)
    logits = jnp.dot(final, head_wide, precision=exact)
    top = jnp.max(logits, axis=-1, keepdims=True)
    total_exp = jnp.log(jnp.sum(jnp.exp(logits - top), axis=-1, keepdims=True)) + top
    labels = (teacher_bins[:, None] == jnp.arange(bins, dtype=jnp.int32)[None, :]).astype(F32)
    loss_here = total_exp - jnp.sum(logits * labels, axis=-1, keepdims=True)
    g_logits = (jnp.exp(logits - total_exp) - labels) / groups
    g_final = jnp.dot(g_logits, head_wide.T, precision=exact)
    per_token = final_back(g_final)[0] / count
    rounded = per_token.astype(BF).astype(F32)
    g_hidden = jnp.einsum(
        "ojd,jfd->of",
        rounded.reshape(1, groups, d_local),
        down_full.astype(F32),
        precision=exact,
    )

    packed = jnp.concatenate(
        [hidden_sum, rounded, final, g_logits, jnp.broadcast_to(loss_here, (1, 128))], axis=1
    )
    every = gather_all(packed, "dp", groups, 5)[:, 0]
    hidden_every = every[:, :f_local]
    rounded_every = every[:, f_local : f_local + width]
    final_every = every[:, f_local + width : f_local + 2 * width]
    rest = every[:, f_local + 2 * width :]
    loss = jnp.sum(rest[:, bins]) / groups
    mine = group * d_local
    over_seqs = (((0,), (0,)), ((), ()))
    down_weight_gradient = lax.dot_general(
        hidden_every,
        lax.dynamic_slice_in_dim(rounded_every, mine, d_local, axis=1),
        over_seqs,
        precision=exact,
    )
    grad_head = lax.dot_general(
        lax.dynamic_slice_in_dim(final_every, mine, d_local, axis=1),
        rest[:, :bins],
        over_seqs,
        precision=exact,
    )

    up_base = lax.dot_general(normed_two, slope, over_seqs, preferred_element_type=F32)
    up_weight_gradient = lax.psum_scatter(
        (up_base * g_hidden).astype(BF), "dp", scatter_dimension=0, tiled=True
    ).astype(F32)
    g_pre = (slope.astype(F32) * g_hidden).astype(BF)
    g_normed = lax.dot_general(
        g_pre, up_full, (((1,), (1,)), ((), ())), preferred_element_type=F32
    )
    g_second = (
        norm_back(g_normed)[0] + live[:, None] * (per_token / ranks)
    ).astype(BF)
    spread = lax.dot_general(
        out_full, g_second, (((1,), (1,)), ((), ())), preferred_element_type=F32
    ).astype(BF)
    g_context = reduce_scatter(spread.reshape(ranks, e_local, span), "tensor", ranks, 6)
    out_term = (
        jnp.dot(context_all, g_second, preferred_element_type=F32)
        .astype(BF)
        .reshape(ranks, e_local, groups, d_local)
        .transpose(0, 2, 1, 3)
        .reshape(ranks * groups, e_local, d_local)
    )
    output_weight_gradient = lax.psum_scatter(
        out_term, ("tensor", "dp"), scatter_dimension=0, tiled=False
    ).astype(F32)
    g_qkv = attend_back(qkv, lengths, lse, g_context, chunk).reshape(3 * e_local, span)
    qkv_term = lax.dot_general(
        normed_one, g_qkv, (((0,), (1,)), ((), ())), preferred_element_type=F32
    )
    query_key_value_gradient = (
        lax.psum_scatter(qkv_term.astype(BF), "dp", scatter_dimension=0, tiled=True)
        .astype(F32)
        .reshape(d_local, 3, e_local)
    )
    return (
        loss,
        query_key_value_gradient,
        output_weight_gradient,
        up_weight_gradient,
        down_weight_gradient,
        grad_head,
    )


def solution(mesh):
    placed = (
        P("dp", "tensor"),
        P("dp"),
        P("dp"),
        P("tensor", None),
        P("dp", None, "tensor"),
        P("tensor", "dp"),
        P("dp", "tensor"),
        P("tensor", "dp"),
        P("dp", None),
    )
    return jax.shard_map(
        per_device,
        mesh=mesh,
        in_specs=placed,
        out_specs=(
            P(),
            P("dp", None, "tensor"),
            P("tensor", "dp"),
            P("dp", "tensor"),
            P("tensor", "dp"),
            P("dp", None),
        ),
        check_vma=False,
    )
```

```python
import functools

import jax
import jax.numpy as jnp
from jax import lax
from jax.experimental import pallas as pl
from jax.experimental.pallas import tpu as pltpu
from jax.sharding import PartitionSpec as P

HEAD_WIDTH = 64
EPS = 1e-05
BF = jnp.bfloat16
F32 = jnp.float32
MESH = pl.DeviceIdType.MESH
VMEM = pltpu.VMEM
BIG = 60 * 1024 * 1024


def normalize(values):
    mean = jnp.mean(values, axis=-1, keepdims=True)
    centered = values - mean
    return centered * lax.rsqrt(jnp.mean(centered * centered, axis=-1, keepdims=True) + EPS)


def vmem_spec():
    return pl.BlockSpec(memory_space=pltpu.VMEM)


def greet(axis, count):
    me = lax.axis_index(axis)
    barrier = pltpu.get_barrier_semaphore()
    for step in range(1, count):
        pl.semaphore_signal(
            barrier, inc=1, device_id={axis: lax.rem(me + step, count)}, device_id_type=MESH
        )
    pl.semaphore_wait(barrier, count - 1)
    return me


def gather_body(axis, count, x_ref, out_ref, send_sem, recv_sem):
    me = greet(axis, count)
    copies = []
    for step in range(1, count):
        copy = pltpu.make_async_remote_copy(
            src_ref=x_ref,
            dst_ref=out_ref.at[me],
            send_sem=send_sem.at[step - 1],
            recv_sem=recv_sem.at[step - 1],
            device_id={axis: lax.rem(me + step, count)},
            device_id_type=MESH,
        )
        copy.start()
        copies.append(copy)
    out_ref[me] = x_ref[...]
    for copy in copies:
        copy.wait()


def gather_all(x, axis, count, ident):
    return pl.pallas_call(
        functools.partial(gather_body, axis, count),
        out_shape=jax.ShapeDtypeStruct((count,) + x.shape, x.dtype),
        in_specs=[vmem_spec()],
        out_specs=vmem_spec(),
        scratch_shapes=[
            pltpu.SemaphoreType.DMA((count - 1,)),
            pltpu.SemaphoreType.DMA((count - 1,)),
        ],
        compiler_params=pltpu.CompilerParams(collective_id=ident, has_side_effects=True),
        name="gather_all",
    )(x)


def scatter_copies(axis, count, me, x_ref, held, send_sem, recv_sem):
    copies = []
    for step in range(1, count):
        peer = lax.rem(me + step, count)
        copies.append(
            pltpu.make_async_remote_copy(
                src_ref=x_ref.at[peer],
                dst_ref=held.at[step - 1],
                send_sem=send_sem.at[step - 1],
                recv_sem=recv_sem.at[step - 1],
                device_id={axis: peer},
                device_id_type=MESH,
            )
        )
    return copies


def scatter_start(*args):
    for copy in scatter_copies(*args):
        copy.start()


def scatter_finish(axis, count, me, x_ref, held, send_sem, recv_sem, put):
    for copy in scatter_copies(axis, count, me, x_ref, held, send_sem, recv_sem):
        copy.wait()

    def body(at):
        total = x_ref[me, at].astype(F32)
        for step in range(1, count):
            total = total + held[step - 1, at].astype(F32)
        put(at, total)

    add_tiles(x_ref.shape[1], 32, body)


def add_tiles(rows, tile, body):
    def step(index, carry):
        body(pl.ds(pl.multiple_of(index * tile, tile), tile))
        return carry

    lax.fori_loop(0, rows // tile, step, 0)


class GroupSum:
    def __init__(self, x_ref, out_ref, pair, mine, far, sems):
        self.x, self.out, self.pair, self.mine, self.far = x_ref, out_ref, pair, mine, far
        self.sems = sems
        self.groups = x_ref.shape[0]
        self.chips = self.groups // 2
        self.rows = x_ref.shape[1]
        me = lax.axis_index("dp")
        self.core = lax.rem(me, 2)
        self.chip = me // 2
        self.near = self.chip * 2 + 1 - self.core

    @staticmethod
    def scratch(shape, dtype):
        groups, rows, columns = shape
        chips = groups // 2
        return [
            VMEM((chips, rows, columns), dtype),
            VMEM((chips, rows, columns), dtype),
            VMEM((chips - 1, rows, columns), dtype),
            pltpu.SemaphoreType.DMA((chips,)),
            pltpu.SemaphoreType.DMA((chips,)),
            pltpu.SemaphoreType.DMA((chips - 1,)),
            pltpu.SemaphoreType.DMA((chips - 1,)),
        ]

    def signal(self, barrier):
        pl.semaphore_signal(
            barrier, inc=1, device_id={"dp": self.near}, device_id_type=MESH
        )
        for step in range(1, self.chips):
            pl.semaphore_signal(
                barrier, inc=1, device_id={"dp": self.owner(step)}, device_id_type=MESH
            )
        return self.chips

    def owner(self, step):
        return lax.rem(self.chip + step, self.chips) * 2 + self.core

    def pair_copies(self):
        copies = []
        for chip in range(self.chips):
            copies.append(
                pltpu.make_async_remote_copy(
                    src_ref=self.x.at[chip * 2 + 1 - self.core],
                    dst_ref=self.pair.at[chip],
                    send_sem=self.sems[0].at[chip],
                    recv_sem=self.sems[1].at[chip],
                    device_id={"dp": self.near},
                    device_id_type=MESH,
                )
            )
        return copies

    def far_copies(self):
        copies = []
        for step in range(1, self.chips):
            copies.append(
                pltpu.make_async_remote_copy(
                    src_ref=self.mine.at[lax.rem(self.chip + step, self.chips)],
                    dst_ref=self.far.at[step - 1],
                    send_sem=self.sems[2].at[step - 1],
                    recv_sem=self.sems[3].at[step - 1],
                    device_id={"dp": self.owner(step)},
                    device_id_type=MESH,
                )
            )
        return copies

    def start(self):
        for copy in self.pair_copies():
            copy.start()

    def middle(self):
        for copy in self.pair_copies():
            copy.wait()

        for chip in range(self.chips):

            def body(at, chip=chip):
                self.mine[chip, at] = (
                    self.x[chip * 2 + self.core, at].astype(F32)
                    + self.pair[chip, at].astype(F32)
                ).astype(self.mine.dtype)

            add_tiles(self.rows, 32, body)
        for copy in self.far_copies():
            copy.start()

    def finish(self):
        for copy in self.far_copies():
            copy.wait()

        def body(at):
            total = self.mine[self.chip, at].astype(F32)
            for step in range(self.chips - 1):
                total = total + self.far[step, at].astype(F32)
            self.out[at] = total

        add_tiles(self.rows, 32, body)


def scatter_and_group_body(count, x_ref, up_ref, out_ref, up_out, held, send_sem, recv_sem, *rest):
    up = GroupSum(up_ref, up_out, rest[0], rest[1], rest[2], rest[3:])
    barrier = pltpu.get_barrier_semaphore()
    me = lax.axis_index("tensor")
    for step in range(1, count):
        pl.semaphore_signal(
            barrier, inc=1, device_id={"tensor": lax.rem(me + step, count)}, device_id_type=MESH
        )
    told = up.signal(barrier)
    pl.semaphore_wait(barrier, count - 1 + told)

    def put(at, total):
        out_ref[at] = total.astype(out_ref.dtype)

    up.start()
    scatter_start("tensor", count, me, x_ref, held, send_sem, recv_sem)
    up.middle()
    scatter_finish("tensor", count, me, x_ref, held, send_sem, recv_sem, put)
    up.finish()


def scatter_and_group(x, up, count, ident):
    return pl.pallas_call(
        functools.partial(scatter_and_group_body, count),
        out_shape=(
            jax.ShapeDtypeStruct(x.shape[1:], x.dtype),
            jax.ShapeDtypeStruct(up.shape[1:], F32),
        ),
        in_specs=[vmem_spec()] * 2,
        out_specs=(vmem_spec(), vmem_spec()),
        scratch_shapes=[
            VMEM((count - 1,) + x.shape[1:], x.dtype),
            pltpu.SemaphoreType.DMA((count - 1,)),
            pltpu.SemaphoreType.DMA((count - 1,)),
        ]
        + GroupSum.scratch(up.shape, up.dtype),
        compiler_params=pltpu.CompilerParams(
            collective_id=ident, has_side_effects=True, vmem_limit_bytes=BIG
        ),
        name="scatter_and_group",
    )(x, up)


def group_sum_body(number, *refs):
    xs, outs, rest = refs[:number], refs[number : 2 * number], refs[2 * number :]
    sums = [
        GroupSum(x, out, *rest[7 * i : 7 * i + 3], rest[7 * i + 3 : 7 * i + 7])
        for i, (x, out) in enumerate(zip(xs, outs))
    ]
    barrier = pltpu.get_barrier_semaphore()
    pl.semaphore_wait(barrier, sums[0].signal(barrier))
    for one in sums:
        one.start()
    for one in sums:
        one.middle()
    for one in sums:
        one.finish()


def group_sum(arrays, ident):
    number = len(arrays)
    scratch = []
    for array in arrays:
        scratch += GroupSum.scratch(array.shape, array.dtype)
    return pl.pallas_call(
        functools.partial(group_sum_body, number),
        out_shape=tuple(jax.ShapeDtypeStruct(a.shape[1:], F32) for a in arrays),
        in_specs=[vmem_spec()] * number,
        out_specs=(vmem_spec(),) * number,
        scratch_shapes=scratch,
        compiler_params=pltpu.CompilerParams(
            collective_id=ident, has_side_effects=True, vmem_limit_bytes=BIG
        ),
        name="group_sum",
    )(*arrays)


def sum_all_body(axis, count, x_ref, out_ref, held, send_sem, recv_sem, send_two, recv_two):
    me = greet(axis, count)

    def put(at, total):
        out_ref[me, at] = total.astype(out_ref.dtype)

    scatter_start(axis, count, me, x_ref, held, send_sem, recv_sem)
    scatter_finish(axis, count, me, x_ref, held, send_sem, recv_sem, put)
    copies = []
    for step in range(1, count):
        copy = pltpu.make_async_remote_copy(
            src_ref=out_ref.at[me],
            dst_ref=out_ref.at[me],
            send_sem=send_two.at[step - 1],
            recv_sem=recv_two.at[step - 1],
            device_id={axis: lax.rem(me + step, count)},
            device_id_type=MESH,
        )
        copy.start()
        copies.append(copy)
    for copy in copies:
        copy.wait()


def sum_all(x, axis, count, ident):
    return pl.pallas_call(
        functools.partial(sum_all_body, axis, count),
        out_shape=jax.ShapeDtypeStruct(x.shape, x.dtype),
        in_specs=[vmem_spec()],
        out_specs=vmem_spec(),
        scratch_shapes=[VMEM((count - 1,) + x.shape[1:], x.dtype)]
        + [pltpu.SemaphoreType.DMA((count - 1,))] * 4,
        compiler_params=pltpu.CompilerParams(collective_id=ident, has_side_effects=True),
        name="sum_all",
    )(x)


def contract(left, right, dims):
    return lax.dot_general(left, right, ((dims[:1], dims[1:]), ((), ())), preferred_element_type=F32)


def masked_scores(keys, query, length):
    scores = contract(keys, query, (0, 0))
    position = lax.broadcasted_iota(jnp.int32, scores.shape, 0)
    return jnp.where(position < length, scores, -1e30)


def attend_body(chunk, length_ref, qkv_ref, out_ref, lse_ref):
    length = length_ref[0]
    keys, vals = qkv_ref[1], qkv_ref[2]
    scale = HEAD_WIDTH ** (-0.5)
    for at in range(0, qkv_ref.shape[2], chunk):
        query = (qkv_ref[0, :, at : at + chunk].astype(F32) * scale).astype(BF)
        scores = masked_scores(keys, query, length)
        top = jnp.max(scores, axis=0, keepdims=True)
        expo = jnp.exp(scores - top)
        total = jnp.sum(expo, axis=0, keepdims=True)
        mixed = contract(vals, expo.astype(BF), (1, 0))
        out_ref[:, at : at + chunk] = (mixed * (1.0 / total)).astype(BF)
        lse_ref[0, :, at : at + chunk] = top + jnp.log(total)


def attend(qkv, lengths, chunk):
    _, width, length = qkv.shape
    heads = width // HEAD_WIDTH
    return pl.pallas_call(
        functools.partial(attend_body, chunk),
        grid=(heads,),
        out_shape=(
            jax.ShapeDtypeStruct((width, length), BF),
            jax.ShapeDtypeStruct((heads, 1, length), F32),
        ),
        in_specs=[
            pl.BlockSpec(memory_space=pltpu.SMEM),
            pl.BlockSpec((3, HEAD_WIDTH, length), lambda h: (0, h, 0)),
        ],
        out_specs=(
            pl.BlockSpec((HEAD_WIDTH, length), lambda h: (h, 0)),
            pl.BlockSpec((1, 1, length), lambda h: (h, 0, 0)),
        ),
        cost_estimate=pl.CostEstimate(
            flops=4 * width * length * length,
            bytes_accessed=8 * width * length,
            transcendentals=heads * length * length,
        ),
        compiler_params=pltpu.CompilerParams(vmem_limit_bytes=BIG),
        name="attend",
    )(lengths, qkv)


def attend_back_body(
    chunk, ranks, length_ref, qkv_ref, lse_ref, grad_ref, x_ref, out_ref, x_out, held, send_sem, recv_sem
):
    me = lax.axis_index("tensor")
    args = ("tensor", ranks, me, x_ref, held, send_sem, recv_sem)

    @pl.when(pl.program_id(0) == 0)
    def _():
        greet("tensor", ranks)
        scatter_start(*args)

    attend_back_head(chunk, length_ref, qkv_ref, lse_ref, grad_ref, out_ref)

    @pl.when(pl.program_id(0) == pl.num_programs(0) - 1)
    def _():
        piece = x_out.shape[2]

        def put(at, total):
            for group in range(x_out.shape[0]):
                x_out[group, at] = total[:, group * piece : (group + 1) * piece].astype(BF)

        scatter_finish(*args, put)


def attend_back_head(chunk, length_ref, qkv_ref, lse_ref, grad_ref, out_ref):
    length = length_ref[0]
    keys, vals = qkv_ref[1], qkv_ref[2]
    scale = HEAD_WIDTH ** (-0.5)
    span = qkv_ref.shape[2]
    g_keys = jnp.zeros((HEAD_WIDTH, span), F32)
    g_vals = jnp.zeros((HEAD_WIDTH, span), F32)
    for at in range(0, span, chunk):
        here = slice(at, at + chunk)
        query = (qkv_ref[0, :, here].astype(F32) * scale).astype(BF)
        grad = grad_ref[:, here]
        probs = jnp.exp(masked_scores(keys, query, length) - lse_ref[0, :, here])
        g_probs = contract(vals, grad, (0, 0))
        weighted = probs * g_probs
        inner = jnp.sum(weighted, axis=0, keepdims=True)
        g_scores = (weighted - probs * inner).astype(BF)
        out_ref[0, :, here] = (contract(keys, g_scores, (1, 0)) * scale).astype(BF)
        g_keys += contract(query, g_scores, (1, 1))
        g_vals += contract(grad, probs.astype(BF), (1, 1))
    out_ref[1] = g_keys.astype(BF)
    out_ref[2] = g_vals.astype(BF)


def attend_back(qkv, lengths, lse, grad, x, groups, chunk, ident):
    _, width, length = qkv.shape
    heads = width // HEAD_WIDTH
    return pl.pallas_call(
        functools.partial(attend_back_body, chunk, x.shape[0]),
        grid=(heads,),
        out_shape=(
            jax.ShapeDtypeStruct(qkv.shape, BF),
            jax.ShapeDtypeStruct((groups, x.shape[1], x.shape[2] // groups), BF),
        ),
        in_specs=[
            pl.BlockSpec(memory_space=pltpu.SMEM),
            pl.BlockSpec((3, HEAD_WIDTH, length), lambda h: (0, h, 0)),
            pl.BlockSpec((1, 1, length), lambda h: (h, 0, 0)),
            pl.BlockSpec((HEAD_WIDTH, length), lambda h: (h, 0)),
            vmem_spec(),
        ],
        out_specs=(
            pl.BlockSpec((3, HEAD_WIDTH, length), lambda h: (0, h, 0)),
            vmem_spec(),
        ),
        scratch_shapes=[
            VMEM((x.shape[0] - 1,) + x.shape[1:], x.dtype),
            pltpu.SemaphoreType.DMA((x.shape[0] - 1,)),
            pltpu.SemaphoreType.DMA((x.shape[0] - 1,)),
        ],
        cost_estimate=pl.CostEstimate(
            flops=10 * width * length * length,
            bytes_accessed=14 * width * length,
            transcendentals=heads * length * length,
        ),
        compiler_params=pltpu.CompilerParams(
            collective_id=ident, has_side_effects=True, vmem_limit_bytes=BIG
        ),
        name="attend_back",
    )(lengths, qkv, lse, grad, x)


def hidden_body(length_ref, normed_ref, up_ref, slope_ref, sum_ref):
    pre = jnp.dot(normed_ref[...], up_ref[...], preferred_element_type=F32)
    live = lax.broadcasted_iota(jnp.int32, pre.shape, 0) < length_ref[0]
    square = pre * pre
    bend = jnp.tanh(0.7978845608028654 * (pre * (1.0 + 0.044715 * square)))
    half = 0.5 * (1.0 + bend)
    act = (pre * half).astype(BF).astype(F32)
    sum_ref[...] = jnp.sum(jnp.where(live, act, 0.0), axis=0, keepdims=True)
    inner = 0.7978845608028654 * (1.0 + 3 * 0.044715 * square)
    slope = half + 0.5 * pre * (1.0 - bend * bend) * inner
    slope_ref[...] = jnp.where(live, slope, 0.0).astype(BF)


def hidden(normed, up, lengths, chunk):
    length, width = normed.shape
    units = up.shape[1]
    return pl.pallas_call(
        hidden_body,
        grid=(units // chunk,),
        out_shape=(
            jax.ShapeDtypeStruct((length, units), BF),
            jax.ShapeDtypeStruct((1, units), F32),
        ),
        in_specs=[
            pl.BlockSpec(memory_space=pltpu.SMEM),
            pl.BlockSpec((length, width), lambda f: (0, 0)),
            pl.BlockSpec((width, chunk), lambda f: (0, f)),
        ],
        out_specs=(
            pl.BlockSpec((length, chunk), lambda f: (0, f)),
            pl.BlockSpec((1, chunk), lambda f: (0, f)),
        ),
        cost_estimate=pl.CostEstimate(
            flops=2 * length * width * units,
            bytes_accessed=6 * length * units,
            transcendentals=length * units,
        ),
        compiler_params=pltpu.CompilerParams(vmem_limit_bytes=BIG),
        name="hidden",
    )(lengths, normed, up)


def per_device(
    token_ids,
    lengths,
    teacher_bins,
    embed_table,
    query_key_value_matrix,
    output_matrix,
    up_matrix,
    down_matrix,
    w_head,
):
    ranks = lax.axis_size("tensor")
    groups = lax.axis_size("dp")
    rank = lax.axis_index("tensor")
    group = lax.axis_index("dp")
    assert token_ids.shape[0] == 1
    local_len = token_ids.shape[1]
    span = local_len * ranks
    vocab_local, width = embed_table.shape
    d_local, _, e_local = query_key_value_matrix.shape
    f_local = up_matrix.shape[1]
    bins = w_head.shape[1]
    exact = lax.Precision.HIGHEST

    qkv_full = lax.all_gather(
        query_key_value_matrix.reshape(d_local, 3 * e_local), "dp", axis=0, tiled=True
    )
    out_parts = lax.all_gather(output_matrix, ("tensor", "dp"), axis=0, tiled=False)
    out_full = (
        out_parts.reshape(ranks, groups, e_local, d_local)
        .transpose(0, 2, 1, 3)
        .reshape(ranks * e_local, width)
    )
    up_full = lax.all_gather(up_matrix, "dp", axis=0, tiled=True)
    low = lax.all_gather(
        jnp.concatenate([down_matrix, w_head.reshape(bins, d_local)], axis=0), "dp", axis=0, tiled=False
    )
    down_full = low[:, :f_local]
    head_wide = low[:, f_local:].reshape(width, bins).astype(F32)

    all_ids = gather_all(token_ids, "tensor", ranks, 1).reshape(ranks, local_len)
    shifted = all_ids - rank * vocab_local
    inside = (shifted >= 0) & (shifted < vocab_local)
    rows = jnp.take(embed_table, jnp.clip(shifted, 0, vocab_local - 1), axis=0)
    first = sum_all(
        jnp.where(inside[..., None], rows, jnp.zeros((), BF)), "tensor", ranks, 2
    ).reshape(span, width)
    normed_one = normalize(first.astype(F32)).astype(BF)
    qkv = (
        lax.dot_general(qkv_full, normed_one, (((0,), (1,)), ((), ())), preferred_element_type=F32)
        .astype(BF)
        .reshape(3, e_local, span)
    )
    chunk = min(256, span)
    context, lse = attend(qkv, lengths, chunk)
    context_all = gather_all(context, "tensor", ranks, 3).reshape(ranks * e_local, span)
    attn = lax.dot_general(
        context_all, out_full, (((0,), (0,)), ((), ())), preferred_element_type=F32
    )
    second = (first.astype(F32) + attn).astype(BF)
    normed_f, norm_back = jax.vjp(normalize, second.astype(F32))
    normed_two = normed_f.astype(BF)
    slope, hidden_sum = hidden(normed_two, up_full, lengths, min(256, f_local))

    live = (jnp.arange(span, dtype=jnp.int32) < lengths[0]).astype(F32)
    count = lengths.astype(F32)[:, None]
    ffn_part = jnp.einsum(
        "of,jfd->ojd", hidden_sum, down_full.astype(F32), precision=exact
    ).reshape(1, width)
    ffn_all = gather_all(ffn_part, "tensor", ranks, 4)
    second_sum = jnp.sum(second.astype(F32) * live[:, None], axis=0, keepdims=True)
    pooled = (second_sum + jnp.sum(ffn_all, axis=0)) / count
    final, final_back = jax.vjp(normalize, pooled)
    logits = jnp.dot(final, head_wide, precision=exact)
    top = jnp.max(logits, axis=-1, keepdims=True)
    total_exp = jnp.log(jnp.sum(jnp.exp(logits - top), axis=-1, keepdims=True)) + top
    labels = (teacher_bins[:, None] == jnp.arange(bins, dtype=jnp.int32)[None, :]).astype(F32)
    loss_here = total_exp - jnp.sum(logits * labels, axis=-1, keepdims=True)
    g_logits = (jnp.exp(logits - total_exp) - labels) / groups
    g_final = jnp.dot(g_logits, head_wide.T, precision=exact)
    per_token = final_back(g_final)[0] / count
    rounded = per_token.astype(BF).astype(F32)
    g_hidden = jnp.einsum(
        "ojd,jfd->of",
        rounded.reshape(1, groups, d_local),
        down_full.astype(F32),
        precision=exact,
    )

    packed = jnp.concatenate(
        [hidden_sum, rounded, final, g_logits, jnp.broadcast_to(loss_here, (1, 128))], axis=1
    )
    every = gather_all(packed, "dp", groups, 5)[:, 0]
    hidden_every = every[:, :f_local]
    rounded_every = every[:, f_local : f_local + width]
    final_every = every[:, f_local + width : f_local + 2 * width]
    rest = every[:, f_local + 2 * width :]
    loss = jnp.sum(rest[:, bins]) / groups
    mine = group * d_local
    over_seqs = (((0,), (0,)), ((), ()))
    down_weight_gradient = lax.dot_general(
        hidden_every,
        lax.dynamic_slice_in_dim(rounded_every, mine, d_local, axis=1),
        over_seqs,
        precision=exact,
    )
    grad_head = lax.dot_general(
        lax.dynamic_slice_in_dim(final_every, mine, d_local, axis=1),
        rest[:, :bins],
        over_seqs,
        precision=exact,
    )

    up_base = lax.dot_general(normed_two, slope, over_seqs, preferred_element_type=F32)
    up_term = (up_base * g_hidden).astype(BF).reshape(groups, d_local, f_local)
    g_pre = (slope.astype(F32) * g_hidden).astype(BF)
    g_normed = lax.dot_general(
        g_pre, up_full, (((1,), (1,)), ((), ())), preferred_element_type=F32
    )
    g_second = (
        norm_back(g_normed)[0] + live[:, None] * (per_token / ranks)
    ).astype(BF)
    spread = lax.dot_general(
        out_full, g_second, (((1,), (1,)), ((), ())), preferred_element_type=F32
    ).astype(BF)
    g_context, up_weight_gradient = scatter_and_group(
        spread.reshape(ranks, e_local, span), up_term, ranks, 6
    )
    out_term = (
        jnp.dot(context_all, g_second, preferred_element_type=F32)
        .astype(BF)
        .reshape(ranks, e_local, width)
    )
    g_qkv, out_mine = attend_back(qkv, lengths, lse, g_context, out_term, groups, chunk, 7)
    qkv_term = lax.dot_general(
        normed_one,
        g_qkv.reshape(3 * e_local, span),
        (((0,), (1,)), ((), ())),
        preferred_element_type=F32,
    )
    qkv_gradient, output_weight_gradient = group_sum(
        [qkv_term.astype(BF).reshape(groups, d_local, 3 * e_local), out_mine], 8
    )
    query_key_value_gradient = qkv_gradient.reshape(d_local, 3, e_local)
    return (
        loss,
        query_key_value_gradient,
        output_weight_gradient,
        up_weight_gradient,
        down_weight_gradient,
        grad_head,
    )


def solution(mesh):
    placed = (
        P("dp", "tensor"),
        P("dp"),
        P("dp"),
        P("tensor", None),
        P("dp", None, "tensor"),
        P("tensor", "dp"),
        P("dp", "tensor"),
        P("tensor", "dp"),
        P("dp", None),
    )
    return jax.shard_map(
        per_device,
        mesh=mesh,
        in_specs=placed,
        out_specs=(
            P(),
            P("dp", None, "tensor"),
            P("tensor", "dp"),
            P("dp", "tensor"),
            P("tensor", "dp"),
            P("dp", None),
        ),
        check_vma=False,
    )
```

```python
import functools

import jax
import jax.numpy as jnp
from jax import lax
from jax.experimental import pallas as pl
from jax.experimental.pallas import tpu as pltpu
from jax.sharding import PartitionSpec as P

HEAD_WIDTH = 64
EPS = 1e-05
BF = jnp.bfloat16
F32 = jnp.float32
MESH = pl.DeviceIdType.MESH
VMEM = pltpu.VMEM
BIG = 60 * 1024 * 1024


def normalize(values):
    mean = jnp.mean(values, axis=-1, keepdims=True)
    centered = values - mean
    return centered * lax.rsqrt(jnp.mean(centered * centered, axis=-1, keepdims=True) + EPS)


def vmem_spec():
    return pl.BlockSpec(memory_space=pltpu.VMEM)


def greet(axis, count):
    me = lax.axis_index(axis)
    barrier = pltpu.get_barrier_semaphore()
    for step in range(1, count):
        pl.semaphore_signal(
            barrier, inc=1, device_id={axis: lax.rem(me + step, count)}, device_id_type=MESH
        )
    pl.semaphore_wait(barrier, count - 1)
    return me


def gather_body(axis, count, x_ref, out_ref, send_sem, recv_sem):
    me = greet(axis, count)
    copies = []
    for step in range(1, count):
        copy = pltpu.make_async_remote_copy(
            src_ref=x_ref,
            dst_ref=out_ref.at[me],
            send_sem=send_sem.at[step - 1],
            recv_sem=recv_sem.at[step - 1],
            device_id={axis: lax.rem(me + step, count)},
            device_id_type=MESH,
        )
        copy.start()
        copies.append(copy)
    out_ref[me] = x_ref[...]
    for copy in copies:
        copy.wait()


def relay_gather(axis, me, src, out, send_sem, recv_sem):
    across = me + 1 - 2 * lax.rem(me, 2)
    over = lax.rem(me + 2, 4)
    half = src.shape[0] // 2
    low, high = pl.ds(0, half), pl.ds(half, half)

    def copy(index, src_part, block, part, device):
        return pltpu.make_async_remote_copy(
            src_ref=src_part,
            dst_ref=out.at[block, part],
            send_sem=send_sem.at[index],
            recv_sem=recv_sem.at[index],
            device_id={axis: device},
            device_id_type=MESH,
        )

    first_a = copy(0, src.at[low], me, low, across)
    first_b = copy(1, src.at[high], me, high, over)
    second_a = copy(2, src.at[high], me, high, across)
    second_b = copy(3, src.at[low], me, low, over)
    for one in (first_a, first_b, second_a, second_b):
        one.start()
    first_a.wait_recv()
    pass_b = copy(4, out.at[across, low], across, low, over)
    pass_b.start()
    first_b.wait_recv()
    pass_a = copy(5, out.at[over, high], over, high, across)
    pass_a.start()
    second_a.wait_recv()
    second_b.wait_recv()
    pass_b.wait_recv()
    pass_a.wait_recv()
    for one in (first_a, first_b, second_a, second_b, pass_b, pass_a):
        one.wait_send()


def relay_body(axis, x_ref, out_ref, send_sem, recv_sem):
    me = greet(axis, 4)
    relay_gather(axis, me, x_ref, out_ref, send_sem, recv_sem)
    out_ref[me] = x_ref[...]


def gather_blocks(x, axis, count, ident):
    if count != 4:
        return gather_all(x, axis, count, ident)
    return pl.pallas_call(
        functools.partial(relay_body, axis),
        out_shape=jax.ShapeDtypeStruct((count,) + x.shape, x.dtype),
        in_specs=[vmem_spec()],
        out_specs=vmem_spec(),
        scratch_shapes=[pltpu.SemaphoreType.DMA((6,)), pltpu.SemaphoreType.DMA((6,))],
        compiler_params=pltpu.CompilerParams(collective_id=ident, has_side_effects=True),
        name="gather_blocks",
    )(x)


def gather_all(x, axis, count, ident):
    return pl.pallas_call(
        functools.partial(gather_body, axis, count),
        out_shape=jax.ShapeDtypeStruct((count,) + x.shape, x.dtype),
        in_specs=[vmem_spec()],
        out_specs=vmem_spec(),
        scratch_shapes=[
            pltpu.SemaphoreType.DMA((count - 1,)),
            pltpu.SemaphoreType.DMA((count - 1,)),
        ],
        compiler_params=pltpu.CompilerParams(collective_id=ident, has_side_effects=True),
        name="gather_all",
    )(x)


def scatter_copies(axis, count, me, x_ref, held, send_sem, recv_sem):
    copies = []
    for step in range(1, count):
        peer = lax.rem(me + step, count)
        copies.append(
            pltpu.make_async_remote_copy(
                src_ref=x_ref.at[peer],
                dst_ref=held.at[step - 1],
                send_sem=send_sem.at[step - 1],
                recv_sem=recv_sem.at[step - 1],
                device_id={axis: peer},
                device_id_type=MESH,
            )
        )
    return copies


def scatter_start(*args):
    for copy in scatter_copies(*args):
        copy.start()


def scatter_finish(axis, count, me, x_ref, held, send_sem, recv_sem, put):
    for copy in scatter_copies(axis, count, me, x_ref, held, send_sem, recv_sem):
        copy.wait()

    def body(at):
        total = x_ref[me, at].astype(F32)
        for step in range(1, count):
            total = total + held[step - 1, at].astype(F32)
        put(at, total)

    add_tiles(x_ref.shape[1], 32, body)


def add_tiles(rows, tile, body):
    def step(index, carry):
        body(pl.ds(pl.multiple_of(index * tile, tile), tile))
        return carry

    lax.fori_loop(0, rows // tile, step, 0)


class GroupSum:
    def __init__(self, x_ref, out_ref, pair, mine, far, sems):
        self.x, self.out, self.pair, self.mine, self.far = x_ref, out_ref, pair, mine, far
        self.sems = sems
        self.groups = x_ref.shape[0]
        self.chips = self.groups // 2
        self.rows = x_ref.shape[1]
        me = lax.axis_index("dp")
        self.core = lax.rem(me, 2)
        self.chip = me // 2
        self.near = self.chip * 2 + 1 - self.core

    @staticmethod
    def scratch(shape, dtype):
        groups, rows, columns = shape
        chips = groups // 2
        return [
            VMEM((chips, rows, columns), dtype),
            VMEM((chips, rows, columns), dtype),
            VMEM((chips - 1, rows, columns), dtype),
            pltpu.SemaphoreType.DMA((chips,)),
            pltpu.SemaphoreType.DMA((chips,)),
            pltpu.SemaphoreType.DMA((chips - 1,)),
            pltpu.SemaphoreType.DMA((chips - 1,)),
        ]

    def signal(self, barrier):
        pl.semaphore_signal(
            barrier, inc=1, device_id={"dp": self.near}, device_id_type=MESH
        )
        for step in range(1, self.chips):
            pl.semaphore_signal(
                barrier, inc=1, device_id={"dp": self.owner(step)}, device_id_type=MESH
            )
        return self.chips

    def owner(self, step):
        return lax.rem(self.chip + step, self.chips) * 2 + self.core

    def pair_copies(self):
        copies = []
        for chip in range(self.chips):
            copies.append(
                pltpu.make_async_remote_copy(
                    src_ref=self.x.at[chip * 2 + 1 - self.core],
                    dst_ref=self.pair.at[chip],
                    send_sem=self.sems[0].at[chip],
                    recv_sem=self.sems[1].at[chip],
                    device_id={"dp": self.near},
                    device_id_type=MESH,
                )
            )
        return copies

    def far_copies(self):
        copies = []
        for step in range(1, self.chips):
            copies.append(
                pltpu.make_async_remote_copy(
                    src_ref=self.mine.at[lax.rem(self.chip + step, self.chips)],
                    dst_ref=self.far.at[step - 1],
                    send_sem=self.sems[2].at[step - 1],
                    recv_sem=self.sems[3].at[step - 1],
                    device_id={"dp": self.owner(step)},
                    device_id_type=MESH,
                )
            )
        return copies

    def start(self):
        for copy in self.pair_copies():
            copy.start()

    def middle(self):
        for copy in self.pair_copies():
            copy.wait()

        for chip in range(self.chips):

            def body(at, chip=chip):
                self.mine[chip, at] = (
                    self.x[chip * 2 + self.core, at].astype(F32)
                    + self.pair[chip, at].astype(F32)
                ).astype(self.mine.dtype)

            add_tiles(self.rows, 32, body)
        for copy in self.far_copies():
            copy.start()

    def finish(self):
        for copy in self.far_copies():
            copy.wait()

        def body(at):
            total = self.mine[self.chip, at].astype(F32)
            for step in range(self.chips - 1):
                total = total + self.far[step, at].astype(F32)
            self.out[at] = total

        add_tiles(self.rows, 32, body)


def scatter_and_group_body(
    count, x_ref, up_ref, small_ref, out_ref, up_out, small_out, held, send_sem, recv_sem, *rest
):
    up = GroupSum(up_ref, up_out, rest[0], rest[1], rest[2], rest[3:7])
    small_send, small_recv = rest[7:]
    groups = small_out.shape[0]
    group = lax.axis_index("dp")
    barrier = pltpu.get_barrier_semaphore()
    me = lax.axis_index("tensor")
    for step in range(1, count):
        pl.semaphore_signal(
            barrier, inc=1, device_id={"tensor": lax.rem(me + step, count)}, device_id_type=MESH
        )
    for step in range(1, groups):
        pl.semaphore_signal(
            barrier, inc=1, device_id={"dp": lax.rem(group + step, groups)}, device_id_type=MESH
        )
    pl.semaphore_wait(barrier, count + groups - 2)
    smalls = []
    for step in range(1, groups):
        smalls.append(
            pltpu.make_async_remote_copy(
                src_ref=small_ref,
                dst_ref=small_out.at[group],
                send_sem=small_send.at[step - 1],
                recv_sem=small_recv.at[step - 1],
                device_id={"dp": lax.rem(group + step, groups)},
                device_id_type=MESH,
            )
        )

    def put(at, total):
        out_ref[at] = total.astype(out_ref.dtype)

    up.start()
    scatter_start("tensor", count, me, x_ref, held, send_sem, recv_sem)
    up.middle()
    for copy in smalls:
        copy.start()
    small_out[group] = small_ref[...]
    scatter_finish("tensor", count, me, x_ref, held, send_sem, recv_sem, put)
    up.finish()
    for copy in smalls:
        copy.wait()


def scatter_and_group(x, up, small, count, ident):
    return pl.pallas_call(
        functools.partial(scatter_and_group_body, count),
        out_shape=(
            jax.ShapeDtypeStruct(x.shape[1:], x.dtype),
            jax.ShapeDtypeStruct(up.shape[1:], F32),
            jax.ShapeDtypeStruct(up.shape[:1] + small.shape, F32),
        ),
        in_specs=[vmem_spec()] * 3,
        out_specs=(vmem_spec(),) * 3,
        scratch_shapes=[
            VMEM((count - 1,) + x.shape[1:], x.dtype),
            pltpu.SemaphoreType.DMA((count - 1,)),
            pltpu.SemaphoreType.DMA((count - 1,)),
        ]
        + GroupSum.scratch(up.shape, up.dtype)
        + [pltpu.SemaphoreType.DMA((up.shape[0] - 1,))] * 2,
        compiler_params=pltpu.CompilerParams(
            collective_id=ident, has_side_effects=True, vmem_limit_bytes=BIG
        ),
        name="scatter_and_group",
    )(x, up, small)


def group_sum_body(number, *refs):
    xs, outs, rest = refs[:number], refs[number : 2 * number], refs[2 * number :]
    sums = [
        GroupSum(x, out, *rest[7 * i : 7 * i + 3], rest[7 * i + 3 : 7 * i + 7])
        for i, (x, out) in enumerate(zip(xs, outs))
    ]
    barrier = pltpu.get_barrier_semaphore()
    pl.semaphore_wait(barrier, sums[0].signal(barrier))
    for one in sums:
        one.start()
    for one in sums:
        one.middle()
    for one in sums:
        one.finish()


def group_sum(arrays, ident):
    number = len(arrays)
    scratch = []
    for array in arrays:
        scratch += GroupSum.scratch(array.shape, array.dtype)
    return pl.pallas_call(
        functools.partial(group_sum_body, number),
        out_shape=tuple(jax.ShapeDtypeStruct(a.shape[1:], F32) for a in arrays),
        in_specs=[vmem_spec()] * number,
        out_specs=(vmem_spec(),) * number,
        scratch_shapes=scratch,
        compiler_params=pltpu.CompilerParams(
            collective_id=ident, has_side_effects=True, vmem_limit_bytes=BIG
        ),
        name="group_sum",
    )(*arrays)


def sum_all_body(axis, count, x_ref, out_ref, held, send_sem, recv_sem, send_two, recv_two):
    me = greet(axis, count)

    def put(at, total):
        out_ref[me, at] = total.astype(out_ref.dtype)

    scatter_start(axis, count, me, x_ref, held, send_sem, recv_sem)
    scatter_finish(axis, count, me, x_ref, held, send_sem, recv_sem, put)
    if count == 4:
        relay_gather(axis, me, out_ref.at[me], out_ref, send_two, recv_two)
        return
    copies = []
    for step in range(1, count):
        copy = pltpu.make_async_remote_copy(
            src_ref=out_ref.at[me],
            dst_ref=out_ref.at[me],
            send_sem=send_two.at[step - 1],
            recv_sem=recv_two.at[step - 1],
            device_id={axis: lax.rem(me + step, count)},
            device_id_type=MESH,
        )
        copy.start()
        copies.append(copy)
    for copy in copies:
        copy.wait()


def sum_all(x, axis, count, ident):
    return pl.pallas_call(
        functools.partial(sum_all_body, axis, count),
        out_shape=jax.ShapeDtypeStruct(x.shape, x.dtype),
        in_specs=[vmem_spec()],
        out_specs=vmem_spec(),
        scratch_shapes=[VMEM((count - 1,) + x.shape[1:], x.dtype)]
        + [pltpu.SemaphoreType.DMA((count - 1,))] * 2
        + [pltpu.SemaphoreType.DMA((6 if count == 4 else count - 1,))] * 2,
        compiler_params=pltpu.CompilerParams(collective_id=ident, has_side_effects=True),
        name="sum_all",
    )(x)


def contract(left, right, dims):
    return lax.dot_general(left, right, ((dims[:1], dims[1:]), ((), ())), preferred_element_type=F32)


def masked_scores(keys, query, length):
    scores = contract(keys, query, (0, 0))
    position = lax.broadcasted_iota(jnp.int32, scores.shape, 0)
    return jnp.where(position < length, scores, -1e30)


def attend_body(chunk, length_ref, qkv_ref, out_ref, lse_ref):
    length = length_ref[0]
    keys, vals = qkv_ref[1], qkv_ref[2]
    scale = HEAD_WIDTH ** (-0.5)
    for at in range(0, qkv_ref.shape[2], chunk):
        query = (qkv_ref[0, :, at : at + chunk].astype(F32) * scale).astype(BF)
        scores = masked_scores(keys, query, length)
        top = jnp.max(scores, axis=0, keepdims=True)
        expo = jnp.exp(scores - top)
        total = jnp.sum(expo, axis=0, keepdims=True)
        mixed = contract(vals, expo.astype(BF), (1, 0))
        out_ref[:, at : at + chunk] = (mixed * (1.0 / total)).astype(BF)
        lse_ref[0, :, at : at + chunk] = top + jnp.log(total)


def attend(qkv, lengths, chunk):
    _, width, length = qkv.shape
    heads = width // HEAD_WIDTH
    return pl.pallas_call(
        functools.partial(attend_body, chunk),
        grid=(heads,),
        out_shape=(
            jax.ShapeDtypeStruct((width, length), BF),
            jax.ShapeDtypeStruct((heads, 1, length), F32),
        ),
        in_specs=[
            pl.BlockSpec(memory_space=pltpu.SMEM),
            pl.BlockSpec((3, HEAD_WIDTH, length), lambda h: (0, h, 0)),
        ],
        out_specs=(
            pl.BlockSpec((HEAD_WIDTH, length), lambda h: (h, 0)),
            pl.BlockSpec((1, 1, length), lambda h: (h, 0, 0)),
        ),
        cost_estimate=pl.CostEstimate(
            flops=4 * width * length * length,
            bytes_accessed=8 * width * length,
            transcendentals=heads * length * length,
        ),
        compiler_params=pltpu.CompilerParams(vmem_limit_bytes=BIG),
        name="attend",
    )(lengths, qkv)


def attend_back_body(
    chunk, ranks, length_ref, qkv_ref, lse_ref, grad_ref, x_ref, out_ref, x_out, held, send_sem, recv_sem
):
    me = lax.axis_index("tensor")
    args = ("tensor", ranks, me, x_ref, held, send_sem, recv_sem)

    @pl.when(pl.program_id(0) == 0)
    def _():
        greet("tensor", ranks)
        scatter_start(*args)

    attend_back_head(chunk, length_ref, qkv_ref, lse_ref, grad_ref, out_ref)

    @pl.when(pl.program_id(0) == pl.num_programs(0) - 1)
    def _():
        piece = x_out.shape[2]

        def put(at, total):
            for group in range(x_out.shape[0]):
                x_out[group, at] = total[:, group * piece : (group + 1) * piece].astype(BF)

        scatter_finish(*args, put)


def attend_back_head(chunk, length_ref, qkv_ref, lse_ref, grad_ref, out_ref):
    length = length_ref[0]
    keys, vals = qkv_ref[1], qkv_ref[2]
    scale = HEAD_WIDTH ** (-0.5)
    span = qkv_ref.shape[2]
    g_keys = jnp.zeros((HEAD_WIDTH, span), F32)
    g_vals = jnp.zeros((HEAD_WIDTH, span), F32)
    for at in range(0, span, chunk):
        here = slice(at, at + chunk)
        query = (qkv_ref[0, :, here].astype(F32) * scale).astype(BF)
        grad = grad_ref[:, here]
        probs = jnp.exp(masked_scores(keys, query, length) - lse_ref[0, :, here])
        g_probs = contract(vals, grad, (0, 0))
        weighted = probs * g_probs
        inner = jnp.sum(weighted, axis=0, keepdims=True)
        g_scores = (weighted - probs * inner).astype(BF)
        out_ref[0, :, here] = (contract(keys, g_scores, (1, 0)) * scale).astype(BF)
        g_keys += contract(query, g_scores, (1, 1))
        g_vals += contract(grad, probs.astype(BF), (1, 1))
    out_ref[1] = g_keys.astype(BF)
    out_ref[2] = g_vals.astype(BF)


def attend_back(qkv, lengths, lse, grad, x, groups, chunk, ident):
    _, width, length = qkv.shape
    heads = width // HEAD_WIDTH
    return pl.pallas_call(
        functools.partial(attend_back_body, chunk, x.shape[0]),
        grid=(heads,),
        out_shape=(
            jax.ShapeDtypeStruct(qkv.shape, BF),
            jax.ShapeDtypeStruct((groups, x.shape[1], x.shape[2] // groups), BF),
        ),
        in_specs=[
            pl.BlockSpec(memory_space=pltpu.SMEM),
            pl.BlockSpec((3, HEAD_WIDTH, length), lambda h: (0, h, 0)),
            pl.BlockSpec((1, 1, length), lambda h: (h, 0, 0)),
            pl.BlockSpec((HEAD_WIDTH, length), lambda h: (h, 0)),
            vmem_spec(),
        ],
        out_specs=(
            pl.BlockSpec((3, HEAD_WIDTH, length), lambda h: (0, h, 0)),
            vmem_spec(),
        ),
        scratch_shapes=[
            VMEM((x.shape[0] - 1,) + x.shape[1:], x.dtype),
            pltpu.SemaphoreType.DMA((x.shape[0] - 1,)),
            pltpu.SemaphoreType.DMA((x.shape[0] - 1,)),
        ],
        cost_estimate=pl.CostEstimate(
            flops=10 * width * length * length,
            bytes_accessed=14 * width * length,
            transcendentals=heads * length * length,
        ),
        compiler_params=pltpu.CompilerParams(
            collective_id=ident, has_side_effects=True, vmem_limit_bytes=BIG
        ),
        name="attend_back",
    )(lengths, qkv, lse, grad, x)


def hidden_body(length_ref, normed_ref, up_ref, slope_ref, sum_ref):
    pre = jnp.dot(normed_ref[...], up_ref[...], preferred_element_type=F32)
    live = lax.broadcasted_iota(jnp.int32, pre.shape, 0) < length_ref[0]
    square = pre * pre
    bend = jnp.tanh(0.7978845608028654 * (pre * (1.0 + 0.044715 * square)))
    half = 0.5 * (1.0 + bend)
    act = (pre * half).astype(BF).astype(F32)
    sum_ref[...] = jnp.sum(jnp.where(live, act, 0.0), axis=0, keepdims=True)
    inner = 0.7978845608028654 * (1.0 + 3 * 0.044715 * square)
    slope = half + 0.5 * pre * (1.0 - bend * bend) * inner
    slope_ref[...] = jnp.where(live, slope, 0.0).astype(BF)


def hidden(normed, up, lengths, chunk):
    length, width = normed.shape
    units = up.shape[1]
    return pl.pallas_call(
        hidden_body,
        grid=(units // chunk,),
        out_shape=(
            jax.ShapeDtypeStruct((length, units), BF),
            jax.ShapeDtypeStruct((1, units), F32),
        ),
        in_specs=[
            pl.BlockSpec(memory_space=pltpu.SMEM),
            pl.BlockSpec((length, width), lambda f: (0, 0)),
            pl.BlockSpec((width, chunk), lambda f: (0, f)),
        ],
        out_specs=(
            pl.BlockSpec((length, chunk), lambda f: (0, f)),
            pl.BlockSpec((1, chunk), lambda f: (0, f)),
        ),
        cost_estimate=pl.CostEstimate(
            flops=2 * length * width * units,
            bytes_accessed=6 * length * units,
            transcendentals=length * units,
        ),
        compiler_params=pltpu.CompilerParams(vmem_limit_bytes=BIG),
        name="hidden",
    )(lengths, normed, up)


def per_device(
    token_ids,
    lengths,
    teacher_bins,
    embed_table,
    query_key_value_matrix,
    output_matrix,
    up_matrix,
    down_matrix,
    w_head,
):
    ranks = lax.axis_size("tensor")
    groups = lax.axis_size("dp")
    rank = lax.axis_index("tensor")
    group = lax.axis_index("dp")
    assert token_ids.shape[0] == 1
    local_len = token_ids.shape[1]
    span = local_len * ranks
    vocab_local, width = embed_table.shape
    d_local, _, e_local = query_key_value_matrix.shape
    f_local = up_matrix.shape[1]
    bins = w_head.shape[1]
    exact = lax.Precision.HIGHEST

    qkv_full = lax.all_gather(
        query_key_value_matrix.reshape(d_local, 3 * e_local), "dp", axis=0, tiled=True
    )
    out_parts = lax.all_gather(output_matrix, ("tensor", "dp"), axis=0, tiled=False)
    out_full = (
        out_parts.reshape(ranks, groups, e_local, d_local)
        .transpose(0, 2, 1, 3)
        .reshape(ranks * e_local, width)
    )
    up_full = lax.all_gather(up_matrix, "dp", axis=0, tiled=True)
    low = lax.all_gather(
        jnp.concatenate([down_matrix, w_head.reshape(bins, d_local)], axis=0), "dp", axis=0, tiled=False
    )
    down_full = low[:, :f_local]
    head_wide = low[:, f_local:].reshape(width, bins).astype(F32)

    all_ids = gather_all(token_ids, "tensor", ranks, 1).reshape(ranks, local_len)
    shifted = all_ids - rank * vocab_local
    inside = (shifted >= 0) & (shifted < vocab_local)
    rows = jnp.take(embed_table, jnp.clip(shifted, 0, vocab_local - 1), axis=0)
    first = sum_all(
        jnp.where(inside[..., None], rows, jnp.zeros((), BF)), "tensor", ranks, 2
    ).reshape(span, width)
    normed_one = normalize(first.astype(F32)).astype(BF)
    qkv = (
        lax.dot_general(qkv_full, normed_one, (((0,), (1,)), ((), ())), preferred_element_type=F32)
        .astype(BF)
        .reshape(3, e_local, span)
    )
    chunk = min(256, span)
    context, lse = attend(qkv, lengths, chunk)
    context_all = gather_blocks(context, "tensor", ranks, 3).reshape(ranks * e_local, span)
    attn = lax.dot_general(
        context_all, out_full, (((0,), (0,)), ((), ())), preferred_element_type=F32
    )
    second = (first.astype(F32) + attn).astype(BF)
    normed_f, norm_back = jax.vjp(normalize, second.astype(F32))
    normed_two = normed_f.astype(BF)
    slope, hidden_sum = hidden(normed_two, up_full, lengths, min(256, f_local))

    live = (jnp.arange(span, dtype=jnp.int32) < lengths[0]).astype(F32)
    count = lengths.astype(F32)[:, None]
    ffn_part = jnp.einsum(
        "of,jfd->ojd", hidden_sum, down_full.astype(F32), precision=exact
    ).reshape(1, width)
    ffn_all = gather_all(ffn_part, "tensor", ranks, 4)
    second_sum = jnp.sum(second.astype(F32) * live[:, None], axis=0, keepdims=True)
    pooled = (second_sum + jnp.sum(ffn_all, axis=0)) / count
    final, final_back = jax.vjp(normalize, pooled)
    logits = jnp.dot(final, head_wide, precision=exact)
    top = jnp.max(logits, axis=-1, keepdims=True)
    total_exp = jnp.log(jnp.sum(jnp.exp(logits - top), axis=-1, keepdims=True)) + top
    labels = (teacher_bins[:, None] == jnp.arange(bins, dtype=jnp.int32)[None, :]).astype(F32)
    loss_here = total_exp - jnp.sum(logits * labels, axis=-1, keepdims=True)
    g_logits = (jnp.exp(logits - total_exp) - labels) / groups
    g_final = jnp.dot(g_logits, head_wide.T, precision=exact)
    per_token = final_back(g_final)[0] / count
    rounded = per_token.astype(BF).astype(F32)
    g_hidden = jnp.einsum(
        "ojd,jfd->of",
        rounded.reshape(1, groups, d_local),
        down_full.astype(F32),
        precision=exact,
    )

    packed = jnp.concatenate(
        [hidden_sum, rounded, final, g_logits, jnp.broadcast_to(loss_here, (1, 128))], axis=1
    )

    over_seqs = (((0,), (0,)), ((), ()))
    up_base = lax.dot_general(normed_two, slope, over_seqs, preferred_element_type=F32)
    up_term = (up_base * g_hidden).astype(BF).reshape(groups, d_local, f_local)
    g_pre = (slope.astype(F32) * g_hidden).astype(BF)
    g_normed = lax.dot_general(
        g_pre, up_full, (((1,), (1,)), ((), ())), preferred_element_type=F32
    )
    g_second = (
        norm_back(g_normed)[0] + live[:, None] * (per_token / ranks)
    ).astype(BF)
    spread = lax.dot_general(
        out_full, g_second, (((1,), (1,)), ((), ())), preferred_element_type=F32
    ).astype(BF)
    g_context, up_weight_gradient, every = scatter_and_group(
        spread.reshape(ranks, e_local, span), up_term, packed, ranks, 6
    )
    every = every[:, 0]
    hidden_every = every[:, :f_local]
    rounded_every = every[:, f_local : f_local + width]
    final_every = every[:, f_local + width : f_local + 2 * width]
    rest = every[:, f_local + 2 * width :]
    loss = jnp.sum(rest[:, bins]) / groups
    mine = group * d_local
    down_weight_gradient = lax.dot_general(
        hidden_every,
        lax.dynamic_slice_in_dim(rounded_every, mine, d_local, axis=1),
        over_seqs,
        precision=exact,
    )
    grad_head = lax.dot_general(
        lax.dynamic_slice_in_dim(final_every, mine, d_local, axis=1),
        rest[:, :bins],
        over_seqs,
        precision=exact,
    )

    out_term = (
        jnp.dot(context_all, g_second, preferred_element_type=F32)
        .astype(BF)
        .reshape(ranks, e_local, width)
    )
    g_qkv, out_mine = attend_back(qkv, lengths, lse, g_context, out_term, groups, chunk, 7)
    qkv_term = lax.dot_general(
        normed_one,
        g_qkv.reshape(3 * e_local, span),
        (((0,), (1,)), ((), ())),
        preferred_element_type=F32,
    )
    qkv_gradient, output_weight_gradient = group_sum(
        [qkv_term.astype(BF).reshape(groups, d_local, 3 * e_local), out_mine], 8
    )
    query_key_value_gradient = qkv_gradient.reshape(d_local, 3, e_local)
    return (
        loss,
        query_key_value_gradient,
        output_weight_gradient,
        up_weight_gradient,
        down_weight_gradient,
        grad_head,
    )


def solution(mesh):
    placed = (
        P("dp", "tensor"),
        P("dp"),
        P("dp"),
        P("tensor", None),
        P("dp", None, "tensor"),
        P("tensor", "dp"),
        P("dp", "tensor"),
        P("tensor", "dp"),
        P("dp", None),
    )
    return jax.shard_map(
        per_device,
        mesh=mesh,
        in_specs=placed,
        out_specs=(
            P(),
            P("dp", None, "tensor"),
            P("tensor", "dp"),
            P("dp", "tensor"),
            P("tensor", "dp"),
            P("dp", None),
        ),
        check_vma=False,
    )
```
